8 devices in a mesh: dp: 2 (over z, y), cp: 4 (over x, core).
Axes of the slice: x: 2, y: 2, z: 1, core: 2. Of those that a mesh axis runs over, the one named last changes fastest.
Arguments:
- x_seq: bfloat16 [4, 4096, 1024], P('dp', 'cp'), parts along dimension 0
- dy_seq: float32 [4, 4096, 1024], P('dp', 'cp'), parts along dimension 0
- ln1_gain: float32 [1024], replicated
- ln1_bias: float32 [1024], replicated
- ln2_gain: float32 [1024], replicated
- ln2_bias: float32 [1024], replicated
- w_qkv: bfloat16 [1024, 16, 3, 64], replicated
- b_qkv: bfloat16 [16, 3, 64], replicated
- w_out: bfloat16 [1024, 1024], replicated
- b_out: bfloat16 [1024], replicated
- w_up: bfloat16 [1024, 4096], replicated
- b_up: bfloat16 [4096], replicated
- w_down: bfloat16 [4096, 1024], replicated
- b_down: bfloat16 [1024], replicated
Outputs:
- output 1: bfloat16 [4, 4096, 1024], P('dp', 'cp'), parts along dimension 0
- output 2: float32 [4, 4096, 1024], P('dp', 'cp'), parts along dimension 0
- output 3: float32 [2048], P('dp'), parts along dimension 0
- output 4: float32 [2048], P('dp'), parts along dimension 0
- output 5: float32 [2048], P('dp'), parts along dimension 0
- output 6: float32 [2048], P('dp'), parts along dimension 0
- output 7: float32 [2048, 16, 3, 64], P('dp'), parts along dimension 0
- output 8: float32 [32, 3, 64], P('dp'), parts along dimension 0
- output 9: float32 [2048, 1024], P('dp'), parts along dimension 0
- output 10: float32 [2048], P('dp'), parts along dimension 0
- output 11: float32 [2048, 4096], P('dp'), parts along dimension 0
- output 12: float32 [8192], P('dp'), parts along dimension 0
- output 13: float32 [8192, 1024], P('dp'), parts along dimension 0
- output 14: float32 [2048], P('dp'), parts along dimension 0
There are 2 independent parts. The reference program is written for one: setup_inputs(seed, part) draws one part's arguments, and reference() takes and returns one part's arrays. A program takes and returns all parts, laid end to end along the dimension named above; an argument that names none is the same for every part.
All inputs are finite; a program needn't handle non-finite values.
Results may differ from the reference program's by a relative error of at most 0.0164592.
Values are sent between devices in bfloat16 or wider.
A program may use at most 1 GiB of HBM per device.

```python
import math
import jax
import jax.numpy as jnp
from jax import lax

D = 1024
HEADS = 16
HEAD = 64
FF = 4096
BATCH = 2
SEQ = 4096
ROT = HEAD // 4
QBLK = min(SEQ, 128)
EPS = 1e-5
ROPE_BASE = 10000.0
NEG_BIG = -1e30


def setup_inputs(seed: int = 0, part: int = 0) -> dict:
    part_key = jax.random.fold_in(jax.random.key(seed), part)
    act_keys = jax.random.split(part_key, 2)
    weight_keys = jax.random.split(jax.random.key(seed + 1), 12)
    qk_gain = max(math.log(SEQ / 16.0), 1.0) ** 0.25
    col_scale = jnp.array([qk_gain, qk_gain, 1.0], dtype=jnp.float32)[None, None, :, None] * D ** -0.5

    def normal(rand_key, arr_shape):
        return jax.random.normal(rand_key, arr_shape, dtype=jnp.float32)

    return {
        'x_seq': normal(act_keys[0], (BATCH, SEQ, D)).astype(jnp.bfloat16),
        'dy_seq': normal(act_keys[1], (BATCH, SEQ, D)),
        'ln1_gain': 1.0 + 0.3 * normal(weight_keys[0], (D,)),
        'ln1_bias': 0.3 * normal(weight_keys[1], (D,)),
        'ln2_gain': 1.0 + 0.3 * normal(weight_keys[2], (D,)),
        'ln2_bias': 0.3 * normal(weight_keys[3], (D,)),
        'w_qkv': (normal(weight_keys[4], (D, HEADS, 3, HEAD)) * col_scale).astype(jnp.bfloat16),
        'b_qkv': (0.3 * normal(weight_keys[5], (HEADS, 3, HEAD))).astype(jnp.bfloat16),
        'w_out': (2.0 * D ** -0.5 * normal(weight_keys[6], (D, D))).astype(jnp.bfloat16),
        'b_out': (0.3 * normal(weight_keys[7], (D,))).astype(jnp.bfloat16),
        'w_up': (D ** -0.5 * normal(weight_keys[8], (D, FF))).astype(jnp.bfloat16),
        'b_up': (0.3 * normal(weight_keys[9], (FF,))).astype(jnp.bfloat16),
        'w_down': (FF ** -0.5 * normal(weight_keys[10], (FF, D))).astype(jnp.bfloat16),
        'b_down': (0.3 * normal(weight_keys[11], (D,))).astype(jnp.bfloat16),
    }


def as_stored(values_in):
    return values_in + lax.stop_gradient(values_in.astype(jnp.bfloat16).astype(jnp.float32) - values_in)


def layer_norm(row_vals, norm_gain, norm_shift):
    row_mean = jnp.mean(row_vals, axis=-1, keepdims=True)
    centered = row_vals - row_mean
    row_var = jnp.mean(centered * centered, axis=-1, keepdims=True)
    return centered * lax.rsqrt(row_var + EPS) * norm_gain + norm_shift


def rope_tables():
    inv_freq = ROPE_BASE ** (-jnp.arange(0, ROT, 2, dtype=jnp.float32) / ROT)
    angles = jnp.arange(SEQ, dtype=jnp.float32)[:, None] * inv_freq[None, :]
    return jnp.cos(angles), jnp.sin(angles)


def rotary(head_vals, cos_t, sin_t):
    half_rot = ROT // 2
    first_half = head_vals[..., :half_rot]
    second_half = head_vals[..., half_rot:ROT]
    cos_b = cos_t[None, :, None, :]
    sin_b = sin_t[None, :, None, :]
    return jnp.concatenate([first_half * cos_b - second_half * sin_b, second_half * cos_b + first_half * sin_b, head_vals[..., ROT:]], axis=-1)


def causal_attention(q_all, k_all, v_all):
    n_blocks = SEQ // QBLK
    key_pos = jnp.arange(SEQ)

    def one_block(flat_idx):
        b_idx = flat_idx // n_blocks
        q_start = (flat_idx % n_blocks) * QBLK
        q_blk = lax.dynamic_slice(q_all, (b_idx, q_start, 0, 0), (1, QBLK, HEADS, HEAD))[0]
        k_row = lax.dynamic_index_in_dim(k_all, b_idx, axis=0, keepdims=False)
        v_row = lax.dynamic_index_in_dim(v_all, b_idx, axis=0, keepdims=False)
        scores = jnp.einsum('qhe,khe->hqk', q_blk, k_row) * HEAD ** -0.5
        q_pos = q_start + jnp.arange(QBLK)
        scores = jnp.where(key_pos[None, None, :] <= q_pos[None, :, None], scores, NEG_BIG)
        attn_probs = jax.nn.softmax(scores, axis=-1)
        return jnp.einsum('hqk,khe->qhe', attn_probs, v_row)

    block_outs = lax.map(jax.checkpoint(one_block), jnp.arange(BATCH * n_blocks))
    return block_outs.reshape(BATCH, SEQ, HEADS, HEAD)


def layer_forward(x_rows, ln1_gain, ln1_bias, ln2_gain, ln2_bias, w_qkv, b_qkv, w_out, b_out, w_up, b_up, w_down, b_down):
    cos_t, sin_t = rope_tables()
    h_attn = as_stored(layer_norm(x_rows, ln1_gain, ln1_bias))
    qkv_rows = jnp.einsum('bsd,dhce->bshce', h_attn, w_qkv) + b_qkv
    q_all = as_stored(rotary(qkv_rows[:, :, :, 0], cos_t, sin_t))
    k_all = as_stored(rotary(qkv_rows[:, :, :, 1], cos_t, sin_t))
    v_all = as_stored(qkv_rows[:, :, :, 2])
    attn_ctx = as_stored(causal_attention(q_all, k_all, v_all)).reshape(BATCH, SEQ, D)
    attn_proj = jnp.dot(attn_ctx, w_out) + b_out
    h_mlp = as_stored(layer_norm(x_rows, ln2_gain, ln2_bias))
    gelu_out = as_stored(jax.nn.gelu(jnp.dot(h_mlp, w_up) + b_up, approximate=False))
    mlp_proj = jnp.dot(gelu_out, w_down) + b_down
    return x_rows + attn_proj + mlp_proj


def reference(x_seq, dy_seq, ln1_gain, ln1_bias, ln2_gain, ln2_bias, w_qkv, b_qkv, w_out, b_out, w_up, b_up, w_down, b_down):
    y_full, back_fn = jax.vjp(layer_forward, x_seq.astype(jnp.float32), ln1_gain, ln1_bias, ln2_gain, ln2_bias, w_qkv.astype(jnp.float32), b_qkv.astype(jnp.float32), w_out.astype(jnp.float32), b_out.astype(jnp.float32), w_up.astype(jnp.float32), b_up.astype(jnp.float32), w_down.astype(jnp.float32), b_down.astype(jnp.float32))
    grads = back_fn(dy_seq)
    return (y_full.astype(jnp.bfloat16), grads[0], grads[1], grads[2], grads[3], grads[4], grads[5], grads[6], grads[7], grads[8], grads[9], grads[10], grads[11], grads[12])
```

```python
import jax
import jax.numpy as jnp
from jax import lax
from jax.experimental import pallas as pl
from jax.experimental.pallas import tpu as pltpu
from jax.sharding import PartitionSpec as P

EPS = 1e-5
ROPE_BASE = 10000.0
NEG_BIG = -1e30
LOG2E = 1.4426950408889634
HD = 64
BLK = 1024
SUB = 256
BK = 512


def nn_dot(lhs, rhs):
    return lax.dot_general(lhs, rhs, (((1,), (0,)), ((), ())), preferred_element_type=jnp.float32)


def nt_dot(lhs, rhs):
    return lax.dot_general(lhs, rhs, (((1,), (1,)), ((), ())), preferred_element_type=jnp.float32)


def turn(rows, cos_t, sin_t):
    lo, hi = rows[0:8], rows[8:16]
    return jnp.concatenate([lo * cos_t - hi * sin_t, hi * cos_t + lo * sin_t, rows[16:]], axis=0)


def fwd_kernel(n_blk, coef, me_ref, cos_ref, sin_ref, bias_ref, *refs):
    slots = refs[:n_blk]
    qkv_ref, out_ref, lse_ref = refs[n_blk:n_blk + 3]
    ctx_refs = refs[n_blk + 3:2 * n_blk + 3]
    k_nat, s_a, s_b = refs[2 * n_blk + 3:]
    me = me_ref[0]
    bias = bias_ref[...]
    for s in range(n_blk):
        cols = pl.ds(pl.multiple_of(jnp.bitwise_xor(me, s) * BLK, BLK), BLK)
        cos_t, sin_t = cos_ref[:, cols], sin_ref[:, cols]
        rows = slots[s][...] + bias
        q_t = turn(rows[0:HD], cos_t, sin_t)
        k_t = turn(rows[HD:2 * HD], cos_t, sin_t)
        qkv_ref[0, 0:HD, cols] = q_t.astype(jnp.bfloat16)
        qkv_ref[0, HD:2 * HD, cols] = k_t.astype(jnp.bfloat16)
        qkv_ref[0, 2 * HD:3 * HD, cols] = rows[2 * HD:].astype(jnp.bfloat16)
        k_nat[cols, :] = k_t.T.astype(jnp.bfloat16)

    n_sub = BLK // SUB

    def q_cols(q_idx, sub):
        return pl.ds(pl.multiple_of(q_idx * BLK + sub * SUB, SUB), SUB)

    def make(q_idx, k_start, sub, k_len, buf):
        scores = nn_dot(k_nat[pl.ds(pl.multiple_of(k_start, SUB), k_len), :], qkv_ref[0, 0:HD, q_cols(q_idx, sub)])
        return scores

    def put(q_idx, k_start, sub, buf):
        scores = make(q_idx, k_start, sub, BK, buf)
        buf[:, sub * SUB:(sub + 1) * SUB] = scores
        return jnp.max(scores, axis=0, keepdims=True)

    def take(state, top, k_start, scores):
        old_max, tot, acc = state
        new_max = jnp.maximum(old_max, top)
        probs = jnp.exp2((scores - new_max) * coef)
        fade = jnp.exp2((old_max - new_max) * coef)
        tot = tot * fade + jnp.sum(probs, axis=0, keepdims=True)
        v_t = qkv_ref[0, 2 * HD:3 * HD, pl.ds(pl.multiple_of(k_start, SUB), scores.shape[0])]
        acc = acc * fade + nn_dot(v_t, probs.astype(jnp.bfloat16))
        return new_max, tot, acc

    def one_q(q_idx, _):
        base = q_idx * BLK
        tops = tuple(put(q_idx, 0, c, s_a) for c in range(n_sub))
        start = tuple((jnp.full((1, SUB), NEG_BIG, jnp.float32), jnp.zeros((1, SUB), jnp.float32), jnp.zeros((HD, SUB), jnp.float32)) for _ in range(n_sub))

        def pair(j, carry):
            states, tops_a = carry
            k0 = j * (2 * BK)
            tops_b, mid = [], []
            for c in range(n_sub):
                tops_b.append(put(q_idx, k0 + BK, c, s_b))
                mid.append(take(states[c], tops_a[c], k0, s_a[:, c * SUB:(c + 1) * SUB]))
            tops_n, fin = [], []
            for c in range(n_sub):
                tops_n.append(put(q_idx, k0 + 2 * BK, c, s_a))
                fin.append(take(mid[c], tops_b[c], k0 + BK, s_b[:, c * SUB:(c + 1) * SUB]))
            return tuple(fin), tuple(tops_n)

        states, tops = lax.fori_loop(0, q_idx, pair, (start, tops))
        states = list(states)
        tri = lax.broadcasted_iota(jnp.int32, (SUB, SUB), 0) <= lax.broadcasted_iota(jnp.int32, (SUB, SUB), 1)

        def masked(scores):
            return jnp.where(tri, scores, NEG_BIG)

        half = n_sub // 2
        for c in range(n_sub):
            if c < half:
                for r in range(c):
                    part = s_a[r * SUB:(r + 1) * SUB, c * SUB:(c + 1) * SUB]
                    states[c] = take(states[c], jnp.max(part, axis=0, keepdims=True), base + r * SUB, part)
                part = masked(s_a[c * SUB:(c + 1) * SUB, c * SUB:(c + 1) * SUB])
                states[c] = take(states[c], jnp.max(part, axis=0, keepdims=True), base + c * SUB, part)
            else:
                states[c] = take(states[c], tops[c], base, s_a[:, c * SUB:(c + 1) * SUB])
                for r in range(half, c + 1):
                    part = make(q_idx, base + r * SUB, c, SUB, None)
                    if r == c:
                        part = masked(part)
                    states[c] = take(states[c], jnp.max(part, axis=0, keepdims=True), base + r * SUB, part)
        for c in range(n_sub):
            top, tot, acc = states[c]
            outs = acc / tot
            out_ref[0, :, q_cols(q_idx, c)] = outs
            lse_ref[0, :, q_cols(q_idx, c)] = top * coef + jnp.log2(tot)
        return 0

    lax.fori_loop(0, n_blk, one_q, 0)
    for s in range(n_blk):
        cols = pl.ds(pl.multiple_of(jnp.bitwise_xor(me, s) * BLK, BLK), BLK)
        ctx_refs[s][...] = out_ref[0, :, cols].astype(jnp.bfloat16)


def attn_fwd(me, cos_t, sin_t, bias_col, slots, coef):
    n_blk = len(slots)
    rows, toks = slots[0].shape
    heads, batch, seq = rows // (3 * HD), toks // BLK, n_blk * BLK
    n_pair = heads * batch
    full = lambda h, b, me: (0, 0)
    hb = lambda h, b, me: (h, b)
    one = lambda h, b, me: (h * batch + b, 0, 0)
    return pl.pallas_call(
        lambda *refs: fwd_kernel(n_blk, coef, *refs),
        grid_spec=pltpu.PrefetchScalarGridSpec(
            num_scalar_prefetch=1, grid=(heads, batch),
            in_specs=[pl.BlockSpec((8, seq), full), pl.BlockSpec((8, seq), full), pl.BlockSpec((3 * HD, 1), lambda h, b, me: (h, 0))] + [pl.BlockSpec((3 * HD, BLK), hb)] * n_blk,
            out_specs=[pl.BlockSpec((1, 3 * HD, seq), one), pl.BlockSpec((1, HD, seq), one), pl.BlockSpec((1, 1, seq), one)] + [pl.BlockSpec((HD, BLK), hb)] * n_blk,
            scratch_shapes=[pltpu.VMEM((seq, HD), jnp.bfloat16), pltpu.VMEM((BK, BLK), jnp.float32), pltpu.VMEM((BK, BLK), jnp.float32)]),
        out_shape=[jax.ShapeDtypeStruct((n_pair, 3 * HD, seq), jnp.bfloat16), jax.ShapeDtypeStruct((n_pair, HD, seq), jnp.float32), jax.ShapeDtypeStruct((n_pair, 1, seq), jnp.float32)] + [jax.ShapeDtypeStruct((heads * HD, toks), jnp.bfloat16)] * n_blk,
        compiler_params=pltpu.CompilerParams(dimension_semantics=("arbitrary", "arbitrary"), vmem_limit_bytes=48 * 1024 * 1024),
        cost_estimate=pl.CostEstimate(flops=n_pair * seq * seq * 2 * HD * 4, bytes_accessed=60000000, transcendentals=n_pair * seq * seq // 2),
        name="attn_fwd",
    )(me, cos_t, sin_t, bias_col, *slots)


def bwd_kernel(n_blk, coef, scale, me_ref, cos_ref, sin_ref, qkv_ref, out_ref, lse_ref, *refs):
    dctx = refs[:n_blk]
    dqkv_refs = refs[n_blk:2 * n_blk]
    db_ref = refs[2 * n_blk]
    k_nat, v_nat, do_t, delta, dq_acc, dk_acc, dv_acc = refs[2 * n_blk + 1:]
    me = me_ref[0]
    for s in range(n_blk):
        cols = pl.ds(pl.multiple_of(jnp.bitwise_xor(me, s) * BLK, BLK), BLK)
        d_rows = dctx[s][...]
        do_t[:, cols] = d_rows.astype(jnp.bfloat16)
        delta[:, cols] = jnp.sum(d_rows * out_ref[0, :, cols], axis=0, keepdims=True)
        k_nat[cols, :] = qkv_ref[0, HD:2 * HD, cols].T
        v_nat[cols, :] = qkv_ref[0, 2 * HD:3 * HD, cols].T
    dq_acc[...] = jnp.zeros_like(dq_acc)
    seq = n_blk * BLK
    n_k = seq // BK

    def tile(k_start, k_len, q_start, q_len, mask):
        k_sl = pl.ds(pl.multiple_of(k_start, SUB), k_len)
        q_sl = pl.ds(pl.multiple_of(q_start, SUB), q_len)
        q_t = qkv_ref[0, 0:HD, q_sl]
        g_t = do_t[:, q_sl]
        scores = nn_dot(k_nat[k_sl, :], q_t)
        d_probs = nn_dot(v_nat[k_sl, :], g_t)
        probs = jnp.exp2(scores * coef - lse_ref[0, :, q_sl])
        if mask is not None:
            probs = jnp.where(mask, probs, 0.0)
        d_scores = (probs * (d_probs - delta[:, q_sl])).astype(jnp.bfloat16)
        dv = nt_dot(g_t, probs.astype(jnp.bfloat16))
        dk = nt_dot(q_t, d_scores)
        dq_acc[:, q_sl] += nn_dot(qkv_ref[0, HD:2 * HD, k_sl], d_scores)
        return dk, dv

    tri = lax.broadcasted_iota(jnp.int32, (SUB, SUB), 0) <= lax.broadcasted_iota(jnp.int32, (SUB, SUB), 1)

    def one_k(j, _):
        base = j * BK
        dk0, dv0 = tile(base, SUB, base, SUB, tri)
        dk1, dv1 = tile(base + SUB, SUB, base + SUB, SUB, tri)
        dk2, dv2 = tile(base, SUB, base + SUB, SUB, None)
        start = (jnp.concatenate([dk0 + dk2, dk1], axis=1), jnp.concatenate([dv0 + dv2, dv1], axis=1))

        def one_q(i, carry):
            dk, dv = carry
            for c in range(BK // SUB):
                g_k, g_v = tile(base, BK, i * BK + c * SUB, SUB, None)
                dk, dv = dk + g_k, dv + g_v
            return dk, dv

        dk, dv = lax.fori_loop(j + 1, n_k, one_q, start)
        k_sl = pl.ds(pl.multiple_of(base, BK), BK)
        dk_acc[:, k_sl] = dk
        dv_acc[:, k_sl] = dv
        return 0

    lax.fori_loop(0, n_k, one_k, 0)
    lanes = jnp.zeros((3 * HD, 128), jnp.float32)
    for s in range(n_blk):
        cols = pl.ds(pl.multiple_of(jnp.bitwise_xor(me, s) * BLK, BLK), BLK)
        cos_t, sin_t = cos_ref[:, cols], -sin_ref[:, cols]
        g = jnp.concatenate([turn(dq_acc[:, cols] * scale, cos_t, sin_t), turn(dk_acc[:, cols] * scale, cos_t, sin_t), dv_acc[:, cols]], axis=0)
        dqkv_refs[s][...] = g.astype(jnp.bfloat16)
        for c in range(BLK // 128):
            lanes += g[:, c * 128:(c + 1) * 128]
    db_ref[0] = lanes


def attn_bwd(me, cos_t, sin_t, qkv, outs, lse, dctx, coef, scale, h_from, h_cnt):
    n_blk = len(dctx)
    rows, toks = dctx[0].shape
    batch, seq = toks // BLK, n_blk * BLK
    full = lambda h, b, me: (0, 0)
    hb_in = lambda h, b, me: (h + h_from, b)
    hb = lambda h, b, me: (h, b)
    one = lambda h, b, me: ((h + h_from) * batch + b, 0, 0)
    n_pair = h_cnt * batch
    return pl.pallas_call(
        lambda *refs: bwd_kernel(n_blk, coef, scale, *refs),
        grid_spec=pltpu.PrefetchScalarGridSpec(
            num_scalar_prefetch=1, grid=(h_cnt, batch),
            in_specs=[pl.BlockSpec((8, seq), full), pl.BlockSpec((8, seq), full), pl.BlockSpec((1, 3 * HD, seq), one), pl.BlockSpec((1, HD, seq), one), pl.BlockSpec((1, 1, seq), one)] + [pl.BlockSpec((HD, BLK), hb_in)] * n_blk,
            out_specs=[pl.BlockSpec((3 * HD, BLK), hb)] * n_blk + [pl.BlockSpec((1, 3 * HD, 128), lambda h, b, me: (h * batch + b, 0, 0))],
            scratch_shapes=[pltpu.VMEM((seq, HD), jnp.bfloat16), pltpu.VMEM((seq, HD), jnp.bfloat16), pltpu.VMEM((HD, seq), jnp.bfloat16), pltpu.VMEM((1, seq), jnp.float32)] + [pltpu.VMEM((HD, seq), jnp.float32)] * 3),
        out_shape=[jax.ShapeDtypeStruct((h_cnt * 3 * HD, toks), jnp.bfloat16)] * n_blk + [jax.ShapeDtypeStruct((n_pair, 3 * HD, 128), jnp.float32)],
        compiler_params=pltpu.CompilerParams(dimension_semantics=("arbitrary", "arbitrary"), vmem_limit_bytes=48 * 1024 * 1024),
        cost_estimate=pl.CostEstimate(flops=n_pair * seq * seq * 2 * HD * 10, bytes_accessed=80000000, transcendentals=n_pair * seq * seq // 2),
        name="attn_bwd",
    )(me, cos_t, sin_t, qkv, outs, lse, *dctx)


def norm_parts(rows):
    mean = jnp.mean(rows, axis=-1, keepdims=True)
    centered = rows - mean
    inv_std = lax.rsqrt(jnp.mean(centered * centered, axis=-1, keepdims=True) + EPS)
    return centered * inv_std, inv_std


def norm_backward(d_out, x_norm, inv_std, gain):
    d_norm = d_out * gain
    d_rows = inv_std * (d_norm - jnp.mean(d_norm, axis=-1, keepdims=True) - x_norm * jnp.mean(d_norm * x_norm, axis=-1, keepdims=True))
    return d_rows, jnp.sum(d_out * x_norm, axis=0), jnp.sum(d_out, axis=0)


def dot32(spec, lhs, rhs):
    return jnp.einsum(spec, lhs, rhs, preferred_element_type=jnp.float32)


def exact_gelu(pre_act):
    return jax.nn.gelu(pre_act, approximate=False)


def solution(mesh):
    n_cp = mesh.shape['cp']
    row_spec = P('dp', 'cp', None)
    in_specs = (row_spec, row_spec) + (P(),) * 12
    out_specs = (row_spec, row_spec, P('dp'), P('dp'), P('dp'), P('dp'), P('dp', None, None, None), P('dp', None, None), P('dp', None), P('dp'), P('dp', None), P('dp'), P('dp', None), P('dp'))

    def swap(value, mask):
        return lax.ppermute(value, 'cp', [(i, i ^ mask) for i in range(n_cp)])

    def local_layer(x_blk, dy_blk, ln1_gain, ln1_bias, ln2_gain, ln2_bias, w_qkv, b_qkv, w_out, b_out, w_up, b_up, w_down, b_down):
        batch, row_count, width = x_blk.shape
        heads, hd = w_qkv.shape[1], w_qkv.shape[3]
        ff = w_up.shape[1]
        toks, seq = batch * row_count, n_cp * row_count
        my_heads = heads // n_cp
        q_rows = my_heads * 3 * hd
        c_rows = my_heads * hd
        half = ff // 2
        scale = hd ** -0.5
        coef = scale * LOG2E
        me = lax.axis_index('cp')
        core = me % 2
        slot_of = [jnp.bitwise_xor(me, s) for s in range(n_cp)]
        bf = jnp.bfloat16

        x0 = x_blk.reshape(toks, width)
        dy32 = dy_blk.reshape(toks, width)
        g0 = dy32.astype(bf)
        x2 = swap(x0, 2)
        g2 = swap(g0, 2)
        x1 = swap(x0, 1)
        g1 = swap(g0, 1)
        x3 = swap(x2, 1)
        g3 = swap(g2, 1)
        xs, gs = [x0, x1, x2, x3], [g0, g1, g2, g3]

        w_t = jnp.transpose(w_qkv, (1, 2, 3, 0)).reshape(heads * 3 * hd, width)
        w_t_slot = [lax.dynamic_slice_in_dim(w_t, p * q_rows, q_rows, 0) for p in slot_of]
        w_o_slot = [lax.dynamic_slice_in_dim(w_out, p * c_rows, c_rows, 0) for p in slot_of]
        bias_col = lax.dynamic_slice_in_dim(b_qkv.astype(jnp.float32).reshape(heads * 3 * hd, 1), me * q_rows, q_rows, 0)
        inv_freq = ROPE_BASE ** (-2.0 * jnp.arange(8, dtype=jnp.float32) / 16)
        angles = inv_freq[:, None] * jnp.arange(seq, dtype=jnp.float32)[None, :]
        cos_t, sin_t = jnp.cos(angles), jnp.sin(angles)
        me_arr = me.astype(jnp.int32).reshape(1)

        h_in, m_in = [], []
        for s in range(n_cp):
            x_norm, inv_std = norm_parts(xs[s].astype(jnp.float32))
            h_in.append((x_norm * ln1_gain + ln1_bias).astype(bf))
            m_in.append((x_norm * ln2_gain + ln2_bias).astype(bf))
        slots = [dot32('cd,td->ct', w_t_slot[0], h_in[s]) for s in range(n_cp)]
        fwd = attn_fwd(me_arr, cos_t, sin_t, bias_col, slots, coef)
        qkv, outs, lse, ctx = fwd[0], fwd[1], fwd[2], fwd[3:]
        ctx_got = [ctx[0]] + [swap(ctx[s], s) for s in range(1, n_cp)]

        dctx = [dot32('ce,te->ct', w_o_slot[0], gs[s]) for s in range(n_cp)]
        dq_parts, db_parts = [], []
        for hh in range(my_heads):
            got = attn_bwd(me_arr, cos_t, sin_t, qkv, outs, lse, dctx, coef, scale, hh, 1)
            dq_parts.append(got[:n_cp])
            db_parts.append(jnp.sum(got[n_cp], axis=(0, 2)))
        dq_mine = [jnp.concatenate([dq_parts[hh][s] for hh in range(my_heads)], axis=0) for s in range(n_cp)]
        dq_got = [dq_mine[0]] + [jnp.concatenate([swap(dq_parts[hh][s], s) for hh in range(my_heads)], axis=0) for s in range(1, n_cp)]

        d_w_o = sum(dot32('ct,te->ce', ctx[s], gs[s]) for s in range(n_cp))
        d_w_t = sum(dot32('ct,td->cd', dq_mine[s], h_in[s]) for s in range(n_cp))

        def collect(mine):
            far = swap(mine, 2)
            near, diag = swap(mine, 1), swap(far, 1)
            rows = mine.shape[0]
            full = jnp.zeros((n_cp * rows,) + mine.shape[1:], mine.dtype)
            for s, part in enumerate((mine, near, far, diag)):
                full = lax.dynamic_update_slice_in_dim(full, part, slot_of[s] * rows, 0)
            return full

        d_w_out = collect(d_w_o)
        d_w_qkv_t = collect(d_w_t)
        d_w_qkv = jnp.transpose(d_w_qkv_t.reshape(heads, 3, hd, width), (3, 0, 1, 2))

        w_up_h = lax.dynamic_slice_in_dim(w_up, core * half, half, 1)
        w_down_h = lax.dynamic_slice_in_dim(w_down, core * half, half, 0)
        b_up_h = lax.dynamic_slice_in_dim(b_up, core * half, half, 0).astype(jnp.float32)
        d_w_up_h, d_w_down_h, db_up_h = 0.0, 0.0, 0.0
        mlp_part, dm_part = [], []
        for s in range(n_cp):
            up, = (dot32('td,df->tf', m_in[s], w_up_h) + b_up_h,)
            act, back = jax.vjp(exact_gelu, up)
            act_bf = act.astype(bf)
            d_up = back(dot32('td,fd->tf', gs[s], w_down_h))[0]
            d_up_bf = d_up.astype(bf)
            d_w_down_h += dot32('tf,td->fd', act_bf, gs[s])
            d_w_up_h += dot32('td,tf->df', m_in[s], d_up_bf)
            if s < 2:
                db_up_h += jnp.sum(d_up, axis=0)
                mlp_part.append(dot32('tf,fd->td', act_bf, w_down_h))
                dm_part.append(dot32('tf,df->td', d_up_bf, w_up_h))
        mlp = mlp_part[0] + swap(mlp_part[1], 1)
        d_m = dm_part[0] + swap(dm_part[1], 1)

        def pair_up(mine, axis):
            other = swap(mine, 1)
            shape = list(mine.shape)
            shape[axis] *= 2
            full = jnp.zeros(shape, mine.dtype)
            full = lax.dynamic_update_slice_in_dim(full, mine, core * half, axis)
            return lax.dynamic_update_slice_in_dim(full, other, (1 - core) * half, axis)

        d_w_up = pair_up(d_w_up_h, 1)
        d_w_down = pair_up(d_w_down_h, 0)

        x_rows = x0.astype(jnp.float32)
        proj = sum(dot32('ct,ce->te', ctx_got[s], w_o_slot[s]) for s in range(n_cp))
        y_rows = x_rows + (proj + b_out.astype(jnp.float32)) + (mlp + b_down.astype(jnp.float32))

        d_h = sum(dot32('ct,cd->td', dq_got[s], w_t_slot[s]) for s in range(n_cp))
        x_norm, inv_std = norm_parts(x_rows)
        dx1, dg1, db1 = norm_backward(d_h, x_norm, inv_std, ln1_gain)
        dx2, dg2, db2 = norm_backward(d_m, x_norm, inv_std, ln2_gain)
        dx = dy32 + dx1 + dx2

        db_qkv_mine = jnp.concatenate(db_parts)
        db_qkv = lax.dynamic_update_slice_in_dim(jnp.zeros((heads * 3 * hd,), jnp.float32), db_qkv_mine, me * q_rows, 0)
        db_up = lax.dynamic_update_slice_in_dim(jnp.zeros((ff,), jnp.float32), db_up_h, core * half, 0)
        small = lax.psum(jnp.concatenate([dg1, db1, dg2, db2, jnp.sum(dy32, axis=0), db_qkv, db_up]), 'cp')
        cut = [width, 2 * width, 3 * width, 4 * width, 5 * width, 5 * width + heads * 3 * hd]
        s_g1, s_b1, s_g2, s_b2, s_dy, s_bq, s_bu = jnp.split(small, cut)
        return (y_rows.astype(bf).reshape(x_blk.shape), dx.reshape(dy_blk.shape), s_g1, s_b1, s_g2, s_b2, d_w_qkv, s_bq.reshape(heads, 3, hd), d_w_out, s_dy, d_w_up, s_bu, d_w_down, s_dy)

    return jax.shard_map(local_layer, mesh=mesh, in_specs=in_specs, out_specs=out_specs, check_vma=False)
```

```python
import functools
import jax
import jax.numpy as jnp
from jax import lax
from jax.experimental import pallas as pl
from jax.experimental.pallas import tpu as pltpu
from jax.sharding import PartitionSpec as P

EPS = 1e-5
ROPE_BASE = 10000.0

NEG_BIG = -1e30
LOG2E = 1.4426950408889634
HD = 64
TRIO = 3 * HD
Q_ROWS = slice(HD)
K_ROWS = slice(HD, 2 * HD)
V_ROWS = slice(2 * HD, TRIO)
VMEM_GRANT = 56 << 20
BLK = 1024
SUB = 256
BK = 512


def nn_dot(lhs, rhs):
    return lax.dot_general(lhs, rhs, (((1,), (0,)), ((), ())), preferred_element_type=jnp.float32)


def nt_dot(lhs, rhs):
    return lax.dot_general(lhs, rhs, (((1,), (1,)), ((), ())), preferred_element_type=jnp.float32)


def turn(rows, cos_t, sin_t):
    lo, hi = rows[0:8], rows[8:16]
    return jnp.concatenate([lo * cos_t - hi * sin_t, hi * cos_t + lo * sin_t, rows[16:]], axis=0)


def fwd_kernel(n_blk, coef, me_ref, cos_ref, sin_ref, bias_ref, *refs):
    slots = refs[:n_blk]
    qkv_ref, out_ref, lse_ref = refs[n_blk:n_blk + 3]
    ctx_refs = refs[n_blk + 3:2 * n_blk + 3]
    k_nat, s_a, s_b = refs[2 * n_blk + 3:]
    me = me_ref[0]
    bias = bias_ref[...]
    for s in range(n_blk):
        cols = pl.ds(pl.multiple_of(jnp.bitwise_xor(me, s) * BLK, BLK), BLK)
        cos_t, sin_t = cos_ref[:, cols], sin_ref[:, cols]
        rows = slots[s][...] + bias
        q_t = turn(rows[Q_ROWS], cos_t, sin_t)
        k_t = turn(rows[K_ROWS], cos_t, sin_t)
        qkv_ref[0, Q_ROWS, cols] = q_t.astype(jnp.bfloat16)
        qkv_ref[0, K_ROWS, cols] = k_t.astype(jnp.bfloat16)
        qkv_ref[0, V_ROWS, cols] = rows[V_ROWS].astype(jnp.bfloat16)
        k_nat[cols, :] = k_t.T.astype(jnp.bfloat16)

    n_sub = BLK // SUB

    def q_cols(q_idx, sub):
        return pl.ds(pl.multiple_of(q_idx * BLK + sub * SUB, SUB), SUB)

    def make(q_idx, k_start, sub, k_len):
        scores = nn_dot(k_nat[pl.ds(pl.multiple_of(k_start, SUB), k_len), :], qkv_ref[0, Q_ROWS, q_cols(q_idx, sub)])
        return scores

    def put(q_idx, k_start, sub, buf):
        scores = make(q_idx, k_start, sub, BK)
        buf[:, sub * SUB:(sub + 1) * SUB] = scores
        return jnp.max(scores, axis=0, keepdims=True)

    def take(state, top, k_start, scores):
        old_max, tot, acc = state
        new_max = jnp.maximum(old_max, top)
        probs = jnp.exp2((scores - new_max) * coef)
        fade = jnp.exp2((old_max - new_max) * coef)
        tot = tot * fade + jnp.sum(probs, axis=0, keepdims=True)
        v_t = qkv_ref[0, V_ROWS, pl.ds(pl.multiple_of(k_start, SUB), scores.shape[0])]
        acc = acc * fade + nn_dot(v_t, probs.astype(jnp.bfloat16))
        return new_max, tot, acc

    def one_q(q_idx, _):
        base = q_idx * BLK
        tops = tuple(put(q_idx, 0, c, s_a) for c in range(n_sub))
        start = tuple((jnp.full((1, SUB), NEG_BIG, jnp.float32), jnp.zeros((1, SUB), jnp.float32), jnp.zeros((HD, SUB), jnp.float32)) for _ in range(n_sub))

        def pair(j, carry):
            states, tops_a = carry
            k0 = j * (2 * BK)
            tops_b, mid = [], []
            for c in range(n_sub):
                tops_b.append(put(q_idx, k0 + BK, c, s_b))
                mid.append(take(states[c], tops_a[c], k0, s_a[:, c * SUB:(c + 1) * SUB]))
            tops_n, fin = [], []
            for c in range(n_sub):
                tops_n.append(put(q_idx, k0 + 2 * BK, c, s_a))
                fin.append(take(mid[c], tops_b[c], k0 + BK, s_b[:, c * SUB:(c + 1) * SUB]))
            return tuple(fin), tuple(tops_n)

        states, tops = lax.fori_loop(0, q_idx, pair, (start, tops))
        states = list(states)
        tri = lax.broadcasted_iota(jnp.int32, (SUB, SUB), 0) <= lax.broadcasted_iota(jnp.int32, (SUB, SUB), 1)

        def masked(scores):
            return jnp.where(tri, scores, NEG_BIG)

        half = n_sub // 2
        for c in range(n_sub):
            if c < half:
                for r in range(c):
                    part = s_a[r * SUB:(r + 1) * SUB, c * SUB:(c + 1) * SUB]
                    states[c] = take(states[c], jnp.max(part, axis=0, keepdims=True), base + r * SUB, part)
                part = masked(s_a[c * SUB:(c + 1) * SUB, c * SUB:(c + 1) * SUB])
                states[c] = take(states[c], jnp.max(part, axis=0, keepdims=True), base + c * SUB, part)
            else:
                states[c] = take(states[c], tops[c], base, s_a[:, c * SUB:(c + 1) * SUB])
                for r in range(half, c + 1):
                    part = make(q_idx, base + r * SUB, c, SUB)
                    if r == c:
                        part = masked(part)
                    states[c] = take(states[c], jnp.max(part, axis=0, keepdims=True), base + r * SUB, part)
        for c in range(n_sub):
            top, tot, acc = states[c]
            outs = acc / tot
            out_ref[0, :, q_cols(q_idx, c)] = outs
            lse_ref[0, :, q_cols(q_idx, c)] = top * coef + jnp.log2(tot)
        return 0

    lax.fori_loop(0, n_blk, one_q, 0)
    for s in range(n_blk):
        cols = pl.ds(pl.multiple_of(jnp.bitwise_xor(me, s) * BLK, BLK), BLK)
        ctx_refs[s][...] = out_ref[0, :, cols].astype(jnp.bfloat16)


def attn_fwd(me, cos_t, sin_t, bias_col, slots, coef):
    n_blk = len(slots)
    rows, toks = slots[0].shape
    heads, batch, seq = rows // (TRIO), toks // BLK, n_blk * BLK
    n_pair = heads * batch
    full = lambda h, b, me: (0, 0)
    hb = lambda h, b, me: (h, b)
    one = lambda h, b, me: (h * batch + b, 0, 0)
    return pl.pallas_call(
        lambda *refs: fwd_kernel(n_blk, coef, *refs),
        grid_spec=pltpu.PrefetchScalarGridSpec(
            num_scalar_prefetch=1, grid=(heads, batch),
            in_specs=[*[pl.BlockSpec((8, seq), full)] * 2, pl.BlockSpec((TRIO, 1), lambda h, b, me: (h, 0))] + [pl.BlockSpec((TRIO, BLK), hb)] * n_blk,
            out_specs=[pl.BlockSpec((1, TRIO, seq), one), pl.BlockSpec((1, HD, seq), one), pl.BlockSpec((1, 1, seq), one)] + [pl.BlockSpec((HD, BLK), hb)] * n_blk,
            scratch_shapes=[pltpu.VMEM((seq, HD), jnp.bfloat16), pltpu.VMEM((BK, BLK), jnp.float32), pltpu.VMEM((BK, BLK), jnp.float32)]),
        out_shape=[jax.ShapeDtypeStruct((n_pair, TRIO, seq), jnp.bfloat16), jax.ShapeDtypeStruct((n_pair, HD, seq), jnp.float32), jax.ShapeDtypeStruct((n_pair, 1, seq), jnp.float32)] + [jax.ShapeDtypeStruct((heads * HD, toks), jnp.bfloat16)] * n_blk,
        compiler_params=pltpu.CompilerParams(dimension_semantics=("arbitrary", "arbitrary"), vmem_limit_bytes=VMEM_GRANT),
        cost_estimate=pl.CostEstimate(flops=n_pair * seq * seq * 2 * HD * 4, bytes_accessed=60000000, transcendentals=n_pair * seq * seq // 2),
        name="attn_fwd",
    )(me, cos_t, sin_t, bias_col, *slots)


def bwd_kernel(n_blk, coef, scale, me_ref, cos_ref, sin_ref, qkv_ref, out_ref, lse_ref, *refs):
    dctx = refs[:n_blk]
    dqkv_refs = refs[n_blk:2 * n_blk]
    db_ref = refs[2 * n_blk]
    k_nat, v_nat, do_t, delta, dq_acc, dk_acc, dv_acc, p_s, d_s = refs[2 * n_blk + 1:]
    me = me_ref[0]
    for s in range(n_blk):
        cols = pl.ds(pl.multiple_of(jnp.bitwise_xor(me, s) * BLK, BLK), BLK)
        d_rows = dctx[s][...]
        do_t[:, cols] = d_rows.astype(jnp.bfloat16)
        delta[:, cols] = jnp.sum(d_rows * out_ref[0, :, cols], axis=0, keepdims=True)
        k_nat[cols, :] = qkv_ref[0, K_ROWS, cols].T
        v_nat[cols, :] = qkv_ref[0, V_ROWS, cols].T
    clear(dq_acc, dk_acc, dv_acc)
    lanes_i = lax.broadcasted_iota(jnp.int32, (BK, SUB), 1) - lax.broadcasted_iota(jnp.int32, (BK, SUB), 0)

    def at(start, offset, size):
        return pl.ds(pl.multiple_of(start * BLK + offset, SUB), size)

    def stage1(k_blk, q_blk, r, c, diag):
        shift = c * SUB - r * BK
        k_len = min(BK, shift + SUB) if diag else BK
        q_sl = at(q_blk, c * SUB, SUB)
        k_sl = at(k_blk, r * BK, k_len)
        scores = nn_dot(k_nat[k_sl, :], qkv_ref[0, Q_ROWS, q_sl])
        d_probs = nn_dot(v_nat[k_sl, :], do_t[:, q_sl])
        probs = jnp.exp2(scores * coef - lse_ref[0, :, q_sl])
        if diag and shift < k_len:
            probs = jnp.where(lanes_i[:k_len] >= -shift, probs, 0.0)
        d_scores = (probs * (d_probs - delta[:, q_sl])).astype(jnp.bfloat16)
        rows, cols = slice(r * BK, r * BK + k_len), slice(c * SUB, (c + 1) * SUB)
        p_s[rows, cols] = probs.astype(jnp.bfloat16)
        d_s[rows, cols] = d_scores
        if k_len < BK:
            rest = slice(r * BK + k_len, (r + 1) * BK)
            p_s[rest, cols] = jnp.zeros((BK - k_len, SUB), jnp.bfloat16)
            d_s[rest, cols] = jnp.zeros((BK - k_len, SUB), jnp.bfloat16)

    def stage2(k_blk, q_blk, r, c):
        q_sl = at(q_blk, c * SUB, 2 * SUB)
        k_sl = at(k_blk, r * BK, BK)
        rows, cols = slice(r * BK, (r + 1) * BK), slice(c * SUB, (c + 2) * SUB)
        dv_acc[:, k_sl] += nt_dot(do_t[:, q_sl], p_s[rows, cols])
        dk_acc[:, k_sl] += nt_dot(qkv_ref[0, Q_ROWS, q_sl], d_s[rows, cols])
        dq_acc[:, q_sl] += nn_dot(qkv_ref[0, K_ROWS, k_sl], d_s[rows, cols])

    def body(k_blk, q_blk, diag):
        firsts = [(r, c) for r in range(BLK // BK) for c in range(BLK // SUB) if not diag or (c + 1) * SUB > r * BK]
        ready = []
        for r, c in firsts:
            stage1(k_blk, q_blk, r, c, diag)
            if ready:
                stage2(k_blk, q_blk, *ready.pop(0))
            if c % 2:
                ready.append((r, c - 1))
        for item in ready:
            stage2(k_blk, q_blk, *item)

    def one_k(k_blk, _):
        body(k_blk, k_blk, True)
        lax.fori_loop(k_blk + 1, n_blk, lambda q_blk, c: (body(k_blk, q_blk, False), c)[1], 0)
        return 0

    lax.fori_loop(0, n_blk, one_k, 0)
    lanes = jnp.zeros((TRIO, 128), jnp.float32)
    for s in range(n_blk):
        cols = pl.ds(pl.multiple_of(jnp.bitwise_xor(me, s) * BLK, BLK), BLK)
        cos_t, sin_t = cos_ref[:, cols], -sin_ref[:, cols]
        g = jnp.concatenate([turn(dq_acc[:, cols] * scale, cos_t, sin_t), turn(dk_acc[:, cols] * scale, cos_t, sin_t), dv_acc[:, cols]], axis=0)
        dqkv_refs[s][...] = g.astype(jnp.bfloat16)
        for c in range(BLK // 128):
            lanes += g[:, c * 128:(c + 1) * 128]
    db_ref[0] = lanes


def attn_bwd(me, cos_t, sin_t, qkv, outs, lse, dctx, coef, scale, h_from, h_cnt):
    n_blk = len(dctx)
    _, toks = dctx[0].shape
    batch, seq = toks // BLK, n_blk * BLK
    full = lambda h, b, me: (0, 0)
    hb_in = lambda h, b, me: (h + h_from, b)
    hb = lambda h, b, me: (h, b)
    one = lambda h, b, me: ((h + h_from) * batch + b, 0, 0)
    n_pair = h_cnt * batch
    return pl.pallas_call(
        lambda *refs: bwd_kernel(n_blk, coef, scale, *refs),
        grid_spec=pltpu.PrefetchScalarGridSpec(
            num_scalar_prefetch=1, grid=(h_cnt, batch),
            in_specs=[*[pl.BlockSpec((8, seq), full)] * 2, pl.BlockSpec((1, TRIO, seq), one), pl.BlockSpec((1, HD, seq), one), pl.BlockSpec((1, 1, seq), one)] + [pl.BlockSpec((HD, BLK), hb_in)] * n_blk,
            out_specs=[pl.BlockSpec((TRIO, BLK), hb)] * n_blk + [pl.BlockSpec((1, TRIO, 128), lambda h, b, me: (h * batch + b, 0, 0))],
            scratch_shapes=[pltpu.VMEM((seq, HD), jnp.bfloat16), pltpu.VMEM((seq, HD), jnp.bfloat16), pltpu.VMEM((HD, seq), jnp.bfloat16), pltpu.VMEM((1, seq), jnp.float32)] + [pltpu.VMEM((HD, seq), jnp.float32)] * 3 + [pltpu.VMEM((BLK, BLK), jnp.bfloat16)] * 2),
        out_shape=[jax.ShapeDtypeStruct((h_cnt * TRIO, toks), jnp.bfloat16)] * n_blk + [jax.ShapeDtypeStruct((n_pair, TRIO, 128), jnp.float32)],
        compiler_params=pltpu.CompilerParams(dimension_semantics=("arbitrary", "arbitrary"), vmem_limit_bytes=VMEM_GRANT),
        cost_estimate=pl.CostEstimate(flops=n_pair * seq * seq * 2 * HD * 10, bytes_accessed=80000000, transcendentals=n_pair * seq * seq // 2),
        name="attn_bwd",
    )(me, cos_t, sin_t, qkv, outs, lse, *dctx)


ERFC_P = 0.39
ERFC_C = (0.2353252191761132, 0.09138841398016789, 0.6495594000437396, -0.6354002804457791, 0.8866643709404932, -0.2275371253934527)
GELU_STEP = ERFC_P * 0.5 ** 0.5
TILE = 512
CHUNK = 512
STRIP = 16
PIECE = 256


def gelu_pair(pre):
    step = 1.0 / (1.0 + GELU_STEP * jnp.abs(pre))
    poly = 0.5 * ERFC_C[5]
    for coefficient in ERFC_C[4::-1]:
        poly = poly * step + 0.5 * coefficient
    bell = jnp.exp2(pre * pre * (-0.5 * LOG2E))
    tail = poly * step * bell
    cdf = jnp.where(pre >= 0.0, 1.0 - tail, tail)
    return pre * cdf, cdf + pre * bell * ((2.0 * 3.141592653589793) ** -0.5)


def clear(*refs):
    for ref in refs:
        ref[...] = jnp.zeros_like(ref)


def move(sems, *pairs):
    copies = [pltpu.make_async_copy(src, dst, sems.at[i]) for i, (src, dst) in enumerate(pairs)]
    for copy in copies:
        copy.start()
    for copy in copies:
        copy.wait()


def mlp_kernel(own, n_in, n_tile, core_ref, *refs):
    m_in, g_in = refs[:n_in], refs[n_in:2 * n_in]
    wu, wd, bu = refs[2 * n_in:2 * n_in + 3]
    refs = refs[2 * n_in + 3:]
    if own:
        dwu_out, dwd_out = refs[:2]
        mlp_out, dm_out, db_out = refs[2:2 + n_in], refs[2 + n_in:2 + 2 * n_in], refs[2 + 2 * n_in]
        refs = refs[3 + 2 * n_in:]
    else:
        dwu_in, dwd_in, dwu_full, dwd_full, dwu_out, dwd_out = refs[:6]
        refs = refs[6:]
    m_s, g_s, mt_s, a_s, d_s, at_s, acc_u, acc_d, u_s, v_s, db_s, sems = refs
    step = pl.program_id(0)
    last = n_in * n_tile - 1
    half = wu.shape[1]

    @pl.when(step == 0)
    def _():
        if own:
            clear(acc_u, acc_d, db_out)
        else:
            move(sems, (dwu_in, acc_u), (dwd_in, acc_d))

    for i in range(n_in):
        @pl.when(step // n_tile == i)
        def _(i=i):
            rows = m_in[i][...]
            m_s[...] = rows
            g_s[...] = g_in[i][...]
            mt_s[...] = rows.T

    n_chunk = half // CHUNK

    def first(f):
        def piece(c, is_up):
            inner = slice(c, c + PIECE)
            if is_up:
                u_s[f % 2, :, inner] = nn_dot(m_s[...], wu[:, f * CHUNK + c:f * CHUNK + c + PIECE])
            else:
                v_s[f % 2, :, inner] = nt_dot(g_s[...], wd[f * CHUNK + c:f * CHUNK + c + PIECE, :])

        return [functools.partial(piece, c, is_up) for c in range(0, CHUNK, PIECE) for is_up in (True, False)]

    def middle(f):
        cols = slice(f * CHUNK, (f + 1) * CHUNK)

        def strip(r):
            rows = slice(r, r + STRIP)
            act, slope = gelu_pair(u_s[f % 2, rows, :] + bu[:, cols])
            d_up = v_s[f % 2, rows, :] * slope
            a_s[rows, cols] = act.astype(jnp.bfloat16)
            d_s[rows, cols] = d_up.astype(jnp.bfloat16)
            if own:
                db_s[:, cols] += sum(d_up[q:q + 8] for q in range(0, STRIP, 8))

        return [functools.partial(strip, r) for r in range(0, TILE, STRIP)]

    def turned(f):
        cols = slice(f * CHUNK, (f + 1) * CHUNK)
        at_s[cols, :] = a_s[:, cols].T

    def second(f):
        cols = slice(f * CHUNK, (f + 1) * CHUNK)

        def down(c):
            acc_d[cols, c:c + PIECE] += nn_dot(at_s[cols, :], g_s[:, c:c + PIECE])

        def up(c, r):
            acc_u[r:r + TILE, f * CHUNK + c:f * CHUNK + c + PIECE] += nn_dot(mt_s[r:r + TILE, :], d_s[:, f * CHUNK + c:f * CHUNK + c + PIECE])

        width = m_s.shape[1]
        downs = [functools.partial(down, c) for c in range(0, width, PIECE)]
        return downs + [functools.partial(up, c, r) for r in range(0, width, TILE) for c in range(0, CHUNK, PIECE)]

    if own:
        clear(db_s)
    for t in range(n_chunk + 2):
        mxu = first(t) if t < n_chunk else []
        if t > 1:
            mxu = mxu + second(t - 2)
        vpu = middle(t - 1) if 0 < t <= n_chunk else []
        done = 0
        for i, piece in enumerate(mxu):
            piece()
            upto = len(vpu) * (i + 1) // len(mxu)
            for strip in vpu[done:upto]:
                strip()
            done = upto
        if vpu:
            turned(t - 1)
    if own:
        db_out[...] += jnp.sum(db_s[...], axis=0, keepdims=True)
    if own:
        for i in range(n_in):
            @pl.when(step // n_tile == i)
            def _(i=i):
                mlp_out[i][...] = nn_dot(a_s[...], wd[...])
                dm_out[i][...] = nt_dot(d_s[...], wu[...])

    @pl.when(step == last)
    def _():
        moves = [(acc_u, dwu_out), (acc_d, dwd_out)]
        if not own:
            mine = pl.ds(pl.multiple_of(core_ref[0] * half, half), half)
            moves += [(acc_u, dwu_full.at[:, mine]), (acc_d, dwd_full.at[mine, :])]
        move(sems, *moves)


def mlp_call(own, core, ms, gs, wu, wd, bu, dw=None):
    n_in = len(ms)
    toks, width = ms[0].shape
    half = wu.shape[1] // 2
    n_tile = toks // TILE

    def rows_of(i):
        return pl.BlockSpec((TILE, width), lambda t, core, i=i: (jnp.clip(t - i * n_tile, 0, n_tile - 1), 0))

    keep = lambda t, core: (0, 0)
    once = pl.Buffered(1)
    any_spec = pl.BlockSpec(memory_space=pl.ANY)
    in_specs = [rows_of(i) for i in range(n_in)] * 2 + [pl.BlockSpec((width, half), lambda t, core: (0, core[0]), pipeline_mode=once), pl.BlockSpec((half, width), lambda t, core: (core[0], 0), pipeline_mode=once), pl.BlockSpec((1, half), keep)]
    f32 = jnp.float32
    out_shape = [jax.ShapeDtypeStruct((width, half), f32), jax.ShapeDtypeStruct((half, width), f32)]
    out_specs = [any_spec, any_spec]
    args = [core] + list(ms) + list(gs) + [wu, wd, bu]
    if own:
        out_shape += [jax.ShapeDtypeStruct((toks, width), f32)] * (2 * n_in) + [jax.ShapeDtypeStruct((1, half), f32)]
        out_specs += [rows_of(i) for i in range(n_in)] * 2 + [pl.BlockSpec((1, half), keep)]
    else:
        in_specs += [any_spec, any_spec]
        args += list(dw)
        out_shape = [jax.ShapeDtypeStruct((width, 2 * half), f32), jax.ShapeDtypeStruct((2 * half, width), f32)] + out_shape
        out_specs = [any_spec, any_spec] + out_specs
    bf = jnp.bfloat16
    return pl.pallas_call(
        lambda *refs: mlp_kernel(own, n_in, n_tile, *refs),
        grid_spec=pltpu.PrefetchScalarGridSpec(num_scalar_prefetch=1, grid=(n_in * n_tile,), in_specs=in_specs, out_specs=out_specs, scratch_shapes=[pltpu.VMEM((TILE, width), bf), pltpu.VMEM((TILE, width), bf), pltpu.VMEM((width, TILE), bf), pltpu.VMEM((TILE, half), bf), pltpu.VMEM((TILE, half), bf), pltpu.VMEM((half, TILE), bf), pltpu.VMEM((width, half), f32), pltpu.VMEM((half, width), f32), pltpu.VMEM((2, TILE, CHUNK), f32), pltpu.VMEM((2, TILE, CHUNK), f32), pltpu.VMEM((8, half), f32), pltpu.SemaphoreType.DMA((4,))]),
        out_shape=out_shape,
        compiler_params=pltpu.CompilerParams(dimension_semantics=("arbitrary",), vmem_limit_bytes=66000000),
        cost_estimate=pl.CostEstimate(flops=n_in * toks * width * half * (12 if own else 8), bytes_accessed=80000000, transcendentals=n_in * toks * half * 2),
        name="mlp_own" if own else "mlp_far",
    )(*args)


def norm_rows(rows):
    mean = jnp.mean(rows, axis=-1, keepdims=True)
    centered = rows - mean
    inv_std = lax.rsqrt(jnp.mean(centered * centered, axis=-1, keepdims=True) + EPS)
    return centered * inv_std, inv_std


def prep_kernel(n_in, n_tile, me_ref, *refs):
    x_in = refs[:n_in]
    w_ref, vec_ref = refs[n_in:n_in + 2]
    outs = refs[n_in + 2:]
    for i in range(n_in):
        @pl.when(pl.program_id(0) // n_tile == i)
        def _(i=i):
            x_norm, _ = norm_rows(x_in[i][...].astype(jnp.float32))
            h_bf = (x_norm * vec_ref[0:1, :] + vec_ref[1:2, :]).astype(jnp.bfloat16)
            outs[3 * i][...] = h_bf
            outs[3 * i + 1][...] = (x_norm * vec_ref[2:3, :] + vec_ref[3:4, :]).astype(jnp.bfloat16)
            outs[3 * i + 2][...] = nt_dot(w_ref[...], h_bf)


def clip_rows(i, n_tile):
    return lambda t, me: (jnp.clip(t - i * n_tile, 0, n_tile - 1), 0)


def clip_cols(i, n_tile):
    return lambda t, me: (0, jnp.clip(t - i * n_tile, 0, n_tile - 1))


def prep_call(me, xs, w_t, vecs, q_rows):
    n_in = len(xs)
    toks, width = xs[0].shape
    n_tile = toks // TILE
    bf = jnp.bfloat16
    out_specs, out_shape = [], []
    for i in range(n_in):
        out_specs += [pl.BlockSpec((TILE, width), clip_rows(i, n_tile))] * 2 + [pl.BlockSpec((q_rows, TILE), clip_cols(i, n_tile))]
        out_shape += [jax.ShapeDtypeStruct((toks, width), bf)] * 2 + [jax.ShapeDtypeStruct((q_rows, toks), jnp.float32)]
    got = pl.pallas_call(
        lambda *refs: prep_kernel(n_in, n_tile, *refs),
        grid_spec=pltpu.PrefetchScalarGridSpec(
            num_scalar_prefetch=1, grid=(n_in * n_tile,),
            in_specs=[pl.BlockSpec((TILE, width), clip_rows(i, n_tile)) for i in range(n_in)] + [pl.BlockSpec((q_rows, width), lambda t, me: (me[0], 0)), pl.BlockSpec((4, width), lambda t, me: (0, 0))],
            out_specs=out_specs),
        out_shape=out_shape,
        compiler_params=pltpu.CompilerParams(dimension_semantics=("arbitrary",), vmem_limit_bytes=VMEM_GRANT),
        cost_estimate=pl.CostEstimate(flops=n_in * toks * width * q_rows * 2, bytes_accessed=n_in * 20000000, transcendentals=0),
        name="prep",
    )(me, *xs, w_t, vecs)
    return [got[3 * i:3 * i + 3] for i in range(n_in)]


def wgrad_kernel(n_slot, n_head, n_tile, *refs):
    dq = refs[:n_slot * n_head]
    h_in = refs[n_slot * n_head:n_slot * (n_head + 1)]
    ctx = refs[n_slot * (n_head + 1):n_slot * (n_head + 2)]
    g_in = refs[n_slot * (n_head + 2):n_slot * (n_head + 3)]
    w_out, o_out = refs[n_slot * (n_head + 3):]

    @pl.when(pl.program_id(0) == 0)
    def _():
        clear(w_out, o_out)

    for s in range(n_slot):
        @pl.when(pl.program_id(0) // n_tile == s)
        def _(s=s):
            lhs = jnp.concatenate([dq[s * n_head + hh][...] for hh in range(n_head)], axis=0)
            w_out[...] += nn_dot(lhs, h_in[s][...])
            o_out[...] += nn_dot(ctx[s][...], g_in[s][...])


def wgrad_call(dq, hs, ctx, gs):
    n_slot, n_head = len(dq), len(dq[0])
    toks, width = hs[0].shape
    n_tile = toks // TILE
    rows = TRIO

    def c_spec(s, r):
        return pl.BlockSpec((r, TILE), lambda t, s=s: (0, jnp.clip(t - s * n_tile, 0, n_tile - 1)))

    def r_spec(s):
        return pl.BlockSpec((TILE, width), lambda t, s=s: (jnp.clip(t - s * n_tile, 0, n_tile - 1), 0))

    keep = lambda t: (0, 0)
    sizes = (n_head * rows, n_head * HD)
    return pl.pallas_call(
        lambda *refs: wgrad_kernel(n_slot, n_head, n_tile, *refs),
        grid=(n_slot * n_tile,),
        in_specs=[c_spec(s, rows) for s in range(n_slot) for _ in range(n_head)] + [r_spec(s) for s in range(n_slot)] + [c_spec(s, n_head * HD) for s in range(n_slot)] + [r_spec(s) for s in range(n_slot)],
        out_specs=[pl.BlockSpec((r, width), keep) for r in sizes],
        out_shape=[jax.ShapeDtypeStruct((r, width), jnp.float32) for r in sizes],
        compiler_params=pltpu.CompilerParams(dimension_semantics=("arbitrary",), vmem_limit_bytes=VMEM_GRANT),
        cost_estimate=pl.CostEstimate(flops=n_slot * toks * width * sum(sizes) * 2, bytes_accessed=60000000, transcendentals=0),
        name="wgrad",
    )(*[p for part in dq for p in part], *hs, *ctx, *gs)


FIN = 256


def finish_kernel(n_slot, n_head, me_ref, x_ref, dy_ref, ma_ref, mb_ref, da_ref, db_ref, w_ref, wo_ref, vec_ref, *refs):
    dq = refs[:n_slot * n_head]
    ctx = refs[n_slot * n_head:n_slot * (n_head + 1)]
    y_out, dx_out, sums = refs[n_slot * (n_head + 1):]
    me = me_ref[0]
    width = x_ref.shape[1]
    d_h = jnp.zeros((FIN, width), jnp.float32)
    proj = jnp.zeros((FIN, width), jnp.float32)
    for s in range(n_slot):
        owner = jnp.bitwise_xor(me, s)
        lhs = jnp.concatenate([dq[s * n_head + hh][...] for hh in range(n_head)], axis=0)
        q_rows = n_head * TRIO
        d_h += nn_dot(lhs.T, w_ref[pl.ds(pl.multiple_of(owner * q_rows, q_rows), q_rows), :])
        c_rows = n_head * HD
        proj += nn_dot(ctx[s][...].T, wo_ref[pl.ds(pl.multiple_of(owner * c_rows, c_rows), c_rows), :])
    rows = x_ref[...].astype(jnp.float32)
    y_out[...] = (rows + (proj + vec_ref[2:3, :]) + (ma_ref[...] + mb_ref[...] + vec_ref[3:4, :])).astype(jnp.bfloat16)
    x_norm, inv_std = norm_rows(rows)
    d_m = da_ref[...] + db_ref[...]
    d_norm = d_h * vec_ref[0:1, :] + d_m * vec_ref[1:2, :]
    d_rows = inv_std * (d_norm - jnp.mean(d_norm, axis=-1, keepdims=True) - x_norm * jnp.mean(d_norm * x_norm, axis=-1, keepdims=True))
    dy = dy_ref[...]
    dx_out[...] = dy + d_rows

    @pl.when(pl.program_id(0) == 0)
    def _():
        clear(sums)

    for i, part in enumerate((d_h * x_norm, d_h, d_m * x_norm, d_m, dy)):
        sums[i:i + 1, :] += jnp.sum(part, axis=0, keepdims=True)


def finish_call(me, x0, dy, ma, mb, da, db, w_t, w_out, vecs, dq, ctx):
    n_slot, n_head = len(dq), len(dq[0])
    toks, width = x0.shape
    row = lambda t, me: (t, 0)
    col = lambda t, me: (0, t)
    keep = lambda t, me: (0, 0)
    once = pl.Buffered(1)
    return pl.pallas_call(
        lambda *refs: finish_kernel(n_slot, n_head, *refs),
        grid_spec=pltpu.PrefetchScalarGridSpec(
            num_scalar_prefetch=1, grid=(toks // FIN,),
            in_specs=[pl.BlockSpec((FIN, width), row)] * 6 + [pl.BlockSpec(w_t.shape, keep, pipeline_mode=once), pl.BlockSpec(w_out.shape, keep, pipeline_mode=once), pl.BlockSpec((4, width), keep)] + [pl.BlockSpec((TRIO, FIN), col)] * (n_slot * n_head) + [pl.BlockSpec((n_head * HD, FIN), col)] * n_slot,
            out_specs=[pl.BlockSpec((FIN, width), row), pl.BlockSpec((FIN, width), row), pl.BlockSpec((8, width), keep)]),
        out_shape=[jax.ShapeDtypeStruct((toks, width), jnp.bfloat16), jax.ShapeDtypeStruct((toks, width), jnp.float32), jax.ShapeDtypeStruct((8, width), jnp.float32)],
        compiler_params=pltpu.CompilerParams(dimension_semantics=("arbitrary",), vmem_limit_bytes=VMEM_GRANT),
        cost_estimate=pl.CostEstimate(flops=toks * width * n_head * n_slot * 4 * HD * 2, bytes_accessed=80000000, transcendentals=0),
        name="finish",
    )(me, x0, dy, ma, mb, da, db, w_t, w_out, vecs, *[p for part in dq for p in part], *ctx)


def dot32(spec, lhs, rhs):
    return jnp.einsum(spec, lhs, rhs, preferred_element_type=jnp.float32)


def solution(mesh):
    n_cp = mesh.shape['cp']
    row_spec = P('dp', 'cp')
    in_specs = (row_spec, row_spec) + (P(),) * 12
    out_specs = (row_spec, row_spec, P('dp'), P('dp'), P('dp'), P('dp'), P('dp'), P('dp'), P('dp'), P('dp'), P('dp'), P('dp'), P('dp'), P('dp'))

    def swap(value, mask):
        return lax.ppermute(value, 'cp', [(i, i ^ mask) for i in range(n_cp)])

    def layer_body(x_blk, dy_blk, ln1_gain, ln1_bias, ln2_gain, ln2_bias, w_qkv, b_qkv, w_out, b_out, w_up, b_up, w_down, b_down):
        batch, row_count, width = x_blk.shape
        heads, hd = w_qkv.shape[1], w_qkv.shape[3]
        ff = w_up.shape[1]
        toks, seq = batch * row_count, n_cp * row_count
        my_heads = heads // n_cp
        q_rows = my_heads * 3 * hd
        c_rows = my_heads * hd
        half = ff // 2
        scale = hd ** -0.5
        coef = scale * LOG2E
        me = lax.axis_index('cp')
        core = me % 2
        slot_of = [jnp.bitwise_xor(me, s) for s in range(n_cp)]
        bf, f32 = jnp.bfloat16, jnp.float32
        me_arr = me.astype(jnp.int32).reshape(1)

        x0 = x_blk.reshape(toks, width)
        dy32 = dy_blk.reshape(toks, width)
        x2 = swap(x0, 2)
        x1 = swap(x0, 1)
        g0 = dy32.astype(bf)
        g1 = swap(g0, 1)
        g2 = swap(g0, 2)

        w_t = jnp.transpose(w_qkv, (1, 2, 3, 0)).reshape(heads * 3 * hd, width)
        w_o_mine = lax.dynamic_slice_in_dim(w_out, me * c_rows, c_rows, 0)
        bias_col = lax.dynamic_slice_in_dim(b_qkv.astype(f32).reshape(heads * 3 * hd, 1), me * q_rows, q_rows, 0)
        inv_freq = ROPE_BASE ** (-2.0 * jnp.arange(8, dtype=f32) / 16)
        angles = inv_freq[:, None] * jnp.arange(seq, dtype=f32)[None, :]
        cos_t, sin_t = jnp.cos(angles), jnp.sin(angles)
        vecs = jnp.stack([ln1_gain, ln1_bias, ln2_gain, ln2_bias])
        b_up_h = lax.dynamic_slice_in_dim(b_up, core * half, half, 0).astype(f32).reshape(1, half)
        core_arr = jnp.stack([core.astype(jnp.int32), jnp.int32(1)])

        near = prep_call(me_arr, [x0, x1], w_t, vecs, q_rows)
        dwu, dwd, mlp_0, mlp_1, dm_0, dm_1, db_up_h = mlp_call(True, core_arr, [near[0][1], near[1][1]], [g0, g1], w_up, w_down, b_up_h)
        x2, dwu = lax.optimization_barrier((x2, dwu))
        x3 = swap(x2, 1)
        far = prep_call(me_arr, [x2, x3], w_t, vecs, q_rows)
        mlp_b, dm_b = swap(mlp_1, 1), swap(dm_1, 1)
        h_in = [p[0] for p in near + far]
        fwd = attn_fwd(me_arr, cos_t, sin_t, bias_col, [p[2] for p in near + far], coef)
        qkv, outs, lse, ctx = fwd[0], fwd[1], fwd[2], fwd[3:]
        ctx_got = [ctx[0]] + [swap(ctx[s], s) for s in range(1, n_cp)]

        g2, outs = lax.optimization_barrier((g2, outs))
        g3 = swap(g2, 1)
        gs = [g0, g1, g2, g3]
        dctx = [dot32('ce,te->ct', w_o_mine, gs[s]) for s in range(n_cp)]
        dq_parts, db_parts = [], []
        for hh in range(my_heads):
            got = attn_bwd(me_arr, cos_t, sin_t, qkv, outs, lse, dctx, coef, scale, hh, 1)
            dq_parts.append(got[:n_cp])
            db_parts.append(jnp.sum(got[n_cp], axis=(0, 2)))
        dq_mine = [[dq_parts[hh][s] for hh in range(my_heads)] for s in range(n_cp)]
        dq_got = [dq_mine[0]] + [[swap(part, s) for part in dq_mine[s]] for s in range(1, n_cp)]
        d_w_t, d_w_o = wgrad_call(dq_mine, h_in, ctx, gs)

        far_m, d_w_o, d_w_t = lax.optimization_barrier(([p[1] for p in far], d_w_o, d_w_t))
        dwu_full, dwd_full, dwu_h, dwd_h = mlp_call(False, core_arr, far_m, [g2, g3], w_up, w_down, b_up_h, (dwu, dwd))

        def collect(mine):
            far_part = swap(mine, 2)
            near_part, diag = swap(mine, 1), swap(far_part, 1)
            rows = mine.shape[0]
            full = jnp.zeros((n_cp * rows,) + mine.shape[1:], mine.dtype)
            for s, part in enumerate((mine, near_part, far_part, diag)):
                full = lax.dynamic_update_slice_in_dim(full, part, slot_of[s] * rows, 0)
            return full

        d_w_out = collect(d_w_o)
        d_w_qkv = jnp.transpose(collect(d_w_t).reshape(heads, 3, hd, width), (3, 0, 1, 2))

        x0f, dwu_h, dwd_h = lax.optimization_barrier((x0, dwu_h, dwd_h))
        fin_vecs = jnp.stack([ln1_gain, ln2_gain, b_out.astype(f32), b_down.astype(f32)])
        y_rows, dx, sums = finish_call(me_arr, x0f, dy32, mlp_0, mlp_b, dm_0, dm_b, w_t, w_out, fin_vecs, dq_got, ctx_got)
        d_w_up = lax.dynamic_update_slice_in_dim(dwu_full, swap(dwu_h, 1), (1 - core) * half, 1)
        d_w_down = lax.dynamic_update_slice_in_dim(dwd_full, swap(dwd_h, 1), (1 - core) * half, 0)

        db_qkv = lax.dynamic_update_slice_in_dim(jnp.zeros((heads * 3 * hd,), f32), jnp.concatenate(db_parts), me * q_rows, 0)
        db_up = lax.dynamic_update_slice_in_dim(jnp.zeros((ff,), f32), db_up_h.reshape(half), core * half, 0)
        small = lax.psum(jnp.concatenate([sums[:5].reshape(5 * width), db_qkv, db_up]), 'cp')
        cut = [width, 2 * width, 3 * width, 4 * width, 5 * width, 5 * width + heads * 3 * hd]
        s_g1, s_b1, s_g2, s_b2, s_dy, s_bq, s_bu = jnp.split(small, cut)
        return (y_rows.reshape(x_blk.shape), dx.reshape(dy_blk.shape), s_g1, s_b1, s_g2, s_b2, d_w_qkv, s_bq.reshape(heads, 3, hd), d_w_out, s_dy, d_w_up, s_bu, d_w_down, s_dy)


    return jax.shard_map(layer_body, mesh=mesh, in_specs=in_specs, out_specs=out_specs, check_vma=False)
```
